256 devices in a mesh: blk: 256 (over z, x, y, core).
Axes of the slice: x: 4, y: 4, z: 8, core: 2. Of those that a mesh axis runs over, the one named last changes fastest.
Arguments:
- features: bfloat16 [262144, 128], P('blk'), may hold values from -6 to 6
- lengthscale: float32 [128], replicated, may hold values from 4 to 40
- noise_var: float32 [1], replicated, may hold values from 0.5 to 2
- outputscale: float32 [1], replicated, may hold values from 0.03 to 0.1
- solution: float32 [262144, 64], P('blk'), may hold values from -6 to 6
- residual: float32 [262144, 64], P('blk'), may hold values from -36 to 36
- direction: float32 [262144, 64], P('blk'), may hold values from -36 to 36
Outputs:
- new_solution: float32 [262144, 64], P('blk')
- new_residual: float32 [262144, 64], P('blk')
- new_direction: float32 [262144, 64], P('blk')
The draws below stay inside these ranges and needn't reach their ends.
All inputs are finite; a program needn't handle non-finite values.
Results may differ from the reference program's by a relative error of at most 0.0014.
Values may be sent and summed in bfloat16 or wider, within the bound.
A program may use at most 64 MiB of HBM per device.

```python
import math
import jax
import jax.numpy as jnp
from jax import lax

FEAT = 128
RHS = 64
PTS_DEV = 1024
NPOINTS = 262144
STRIDE_C = 32
STRIDE_D = 65
N_BLK = 256


def rough_field(key, salt):
    first, second = jax.random.split(jax.random.fold_in(key, salt), 2)
    rising = jnp.linspace(1.0, 3.0, NPOINTS, dtype=jnp.float32)[:, None]
    columns = jnp.exp(jax.random.uniform(second, (1, RHS), jnp.float32, jnp.log(0.3), jnp.log(3.0)))
    base = jnp.clip(jax.random.normal(first, (NPOINTS, RHS), jnp.float32), -4.0, 4.0)
    return base * rising * columns


def draw_residual(key, part):
    return rough_field(key, 11)


def draw_direction(key, part):
    return rough_field(key, 23)


def block_scale(rng, dims, shards, least, top_value):
    level, own = 1.0, jax.random.fold_in(rng, 6)
    for axis_at, shards_of in shards:
        heights = jnp.exp(jax.random.uniform(jax.random.fold_in(own, axis_at), (shards_of,), jnp.float32, least / len(shards), top_value / len(shards)))
        level = level * jnp.repeat(heights, dims[axis_at] // shards_of).reshape([-1 if axis == axis_at else 1 for axis in range(len(dims))])
    return level


def normal_values(own_key, extent, width, most, shards=(), held_as=jnp.bfloat16):
    drawn = jax.random.normal(own_key, extent, jnp.float32) * width
    if len(shards) > 0:
        drawn = block_scale(own_key, extent, shards, -0.22, 0.18) * drawn
    return jnp.clip(drawn, min=-most, max=most).astype(held_as)


def setup_inputs(seed: int = 0) -> dict:
    arg_keys = jax.random.split(jax.random.key(seed), 8)
    return {
        "features": normal_values(arg_keys[0], (NPOINTS, FEAT), 1.0, 6.0, ((0, 256),)),
        "lengthscale": jnp.clip(jnp.exp(jax.random.uniform(arg_keys[1], (FEAT,), jnp.float32, math.log(4.0), math.log(40.0))), 4.0, 40.0),
        "noise_var": jnp.clip(jnp.exp(jax.random.uniform(arg_keys[2], (1,), jnp.float32, math.log(0.5), math.log(2.0))), 0.5, 2.0),
        "outputscale": jnp.clip(jnp.exp(jax.random.uniform(arg_keys[3], (1,), jnp.float32, math.log(0.03), math.log(0.1))), 0.03, 0.1),
        "solution": normal_values(arg_keys[4], (NPOINTS, RHS), 1.0, 6.0, ((0, 256),), jnp.float32),
        "residual": draw_residual(jax.random.fold_in(arg_keys[7], 71), 0),
        "direction": draw_direction(jax.random.fold_in(arg_keys[7], 71), 0),
    }


root_five = math.sqrt(5.0)

def matern(left_points, left_norm, right_points, right_norm, scale):
    inner_products = jnp.dot(left_points, right_points.T, preferred_element_type=jnp.float32)
    squared_range = jnp.maximum(left_norm[:, None] + right_norm[None, :] - 2.0 * inner_products, 0.0)
    scaled_range = root_five * jnp.sqrt(squared_range)
    return scale * (1.0 + scaled_range + scaled_range * scaled_range / 3.0) * jnp.exp(-scaled_range)

def reference(features, lengthscale, noise_var, outputscale, solution, residual, direction):
    highest = lax.Precision.HIGHEST
    scaled = (features.astype(jnp.float32) / lengthscale[None, :]).astype(jnp.bfloat16)
    point_norms = lax.optimization_barrier(jnp.sum(jnp.square(scaled.astype(jnp.float32)), axis=1))
    block_points = scaled.reshape(N_BLK, PTS_DEV, FEAT)
    block_norms = point_norms.reshape(N_BLK, PTS_DEV)
    block_direction = direction.reshape(N_BLK, PTS_DEV, RHS)
    scale = outputscale[0]

    def diagonal_block(pieces):
        own_points, own_norm, own_direction = pieces
        kernel_tile = matern(own_points, own_norm, own_points, own_norm, scale)
        return jnp.dot(kernel_tile, own_direction, precision=highest, preferred_element_type=jnp.float32)

    def pair_block(pieces):
        own_points, own_norm, own_direction, far_points, far_norm, far_direction = pieces
        kernel_tile = matern(own_points, own_norm, far_points, far_norm, scale)
        forward = jnp.dot(kernel_tile, far_direction, precision=highest, preferred_element_type=jnp.float32)
        backward = lax.dot_general(kernel_tile, own_direction, (((0,), (0,)), ((), ())), precision=highest, preferred_element_type=jnp.float32)
        return (forward, backward)
    applied = noise_var[0] * block_direction + lax.map(diagonal_block, (block_points, block_norms, block_direction))
    for offset in (1, 3, STRIDE_C, STRIDE_D):
        forward, backward = lax.map(pair_block, (block_points, block_norms, block_direction, jnp.roll(block_points, -offset, 0), jnp.roll(block_norms, -offset, 0), jnp.roll(block_direction, -offset, 0)))
        applied = applied + forward + jnp.roll(backward, offset, 0)
    applied = applied.reshape(NPOINTS, RHS)
    old_norm = lax.optimization_barrier(jnp.sum(residual * residual, axis=0)) / NPOINTS
    curvature = lax.optimization_barrier(jnp.sum(direction * applied, axis=0)) / NPOINTS
    step_size = old_norm / jnp.maximum(curvature, 1.0)
    new_solution = solution + step_size[None, :] * direction
    new_residual = residual - step_size[None, :] * applied
    updated_norm = lax.optimization_barrier(jnp.sum(new_residual * new_residual, axis=0)) / NPOINTS
    new_direction = new_residual + (updated_norm / (old_norm + 1e-06))[None, :] * direction
    return (new_solution, new_residual, new_direction)
```

```python
import math

import jax
import jax.numpy as jnp
from jax import lax
from jax.experimental import pallas as pl
from jax.experimental.pallas import tpu as pltpu
from jax.sharding import PartitionSpec as P

AXIS = "blk"
MESH = pl.DeviceIdType.MESH
OWN, P1, M1, P32, M32, M2, P33 = range(7)
CHUNKS = 4
STRIP = 64

RATE = math.sqrt(10.0) * math.log2(math.e)
POLY_P = 3.0 / math.sqrt(10.0)
POLY_Q = 0.3
TINY = 1e-30


def dot(left, right, dims):
    return lax.dot_general(left, right, (dims, ((), ())), preferred_element_type=jnp.float32)


def kernel(
    n_dev, width, features, lengthscale, noise_var, outputscale, direction, residual,
    applied_ref, coef_ref,
    feat, dvec, res, blk, meta, half_col, dt, s0, s1, t0, t1, rhs, acc, acc2, ret_out, ret_in, sums,
    load_sem, x_send, x_recv, m_send, m_recv, r_send, r_recv, a_send, a_recv,
):
    me = lax.axis_index(AXIS)
    pts = width * CHUNKS
    rhs_n = direction.shape[0]
    s_buf, t_buf = (s0, s1), (t0, t1)

    def at(offset):
        return lax.rem(me + (offset + n_dev), n_dev)

    def group_peer(stride, size, k):
        place = lax.rem(me // stride, size)
        return me + (lax.rem(place + k, size) - place) * stride

    stages = ((1, 8), (8, 4), (32, n_dev // 32))
    loads = [
        pltpu.make_async_copy(features, feat, load_sem.at[0]),
        pltpu.make_async_copy(direction, dvec, load_sem.at[1]),
        pltpu.make_async_copy(residual, res, load_sem.at[2]),
    ]
    for load in loads:
        load.start()

    barrier = pltpu.get_barrier_semaphore()
    peers = [at(o) for o in (1, -1, 2, -2, 32, -32, 33, -33)]
    for stride, size in stages:
        peers += [group_peer(stride, size, k) for k in range(1, size)]
    for peer in peers:
        pl.semaphore_signal(barrier, inc=1, device_id=(peer,), device_id_type=MESH)

    def x_copy(from_slot, to_slot, chunk, way, device):
        rows = pl.ds(pl.multiple_of(chunk * width, width), width)
        return pltpu.make_async_remote_copy(
            src_ref=blk.at[from_slot, :, rows, :],
            dst_ref=blk.at[to_slot, :, rows, :],
            send_sem=x_send.at[way, chunk],
            recv_sem=x_recv.at[to_slot, chunk],
            device_id=(device,),
            device_id_type=MESH,
        )

    def m_copy(from_slot, to_slot, way, device):
        return pltpu.make_async_remote_copy(
            src_ref=meta.at[from_slot],
            dst_ref=meta.at[to_slot],
            send_sem=m_send.at[way],
            recv_sem=m_recv.at[to_slot],
            device_id=(device,),
            device_id_type=MESH,
        )

    own_ways = ((0, OWN, M1, 1), (1, OWN, P32, -32), (2, OWN, M32, 32), (3, OWN, P1, -1))
    fwd_m2 = (4, M1, M2, 1)
    fwd_p33 = (5, P32, P33, -1)

    loads[0].wait()
    scaled = (feat[...].astype(jnp.float32) / lengthscale[...]).astype(jnp.bfloat16)
    blk[OWN, 0] = scaled
    exact = scaled.astype(jnp.float32)
    half = 0.5 * jnp.sum(exact * exact, axis=1, keepdims=True)
    half_col[0] = jnp.broadcast_to(half, (pts, 128))
    for r in range(pts // 128):
        meta[OWN, r : r + 1, :] = half_col[0, r * 128 : (r + 1) * 128, :].T[0:1, :]
    loads[1].wait()
    own_d = dvec[...]
    high = own_d.astype(jnp.bfloat16)
    low = (own_d - high.astype(jnp.float32)).astype(jnp.bfloat16)
    blk[OWN, 1] = jnp.concatenate([high, low], axis=0).T

    pl.semaphore_wait(barrier, len(peers))
    for way, src, dst, offset in own_ways:
        m_copy(src, dst, way, at(offset)).start()
    for chunk in range(CHUNKS):
        for way, src, dst, offset in own_ways:
            x_copy(src, dst, chunk, way, at(offset)).start()

    def gram(left_slot, slot, chunk, par):
        rows = pl.ds(pl.multiple_of(chunk * width, width), width)
        s_buf[par][...] = dot(blk[left_slot, 0], blk[slot, 0, rows, :], ((1,), (1,)))

    def elem(half_slot, slot, chunk, par):
        for h in range(width // 128):
            row = meta[slot, pl.ds(chunk * (width // 128) + h, 1), :]
            for strip in range(pts // STRIP):
                rows = slice(strip * STRIP, (strip + 1) * STRIP)
                lanes = slice(h * 128, (h + 1) * 128)
                u = (half_col[half_slot, rows, :] + row) - s_buf[par][rows, lanes]
                u = jnp.maximum(u, TINY)
                r = u * lax.rsqrt(u)
                value = ((r + POLY_P) * r + POLY_Q) * jnp.exp2(r * (-RATE))
                top = value.astype(jnp.bfloat16)
                rest = (value - top.astype(jnp.float32)).astype(jnp.bfloat16)
                t_buf[par][rows, lanes] = top
                t_buf[par][rows, slice(width + h * 128, width + (h + 1) * 128)] = rest

    def forward(total, slot, chunk, par):
        rows = pl.ds(pl.multiple_of(chunk * width, width), width)
        vec = blk[slot, 1, rows, :]
        lane = lax.broadcasted_iota(jnp.int32, vec.shape, 1)
        top_only = jnp.where(lane < rhs_n, vec.astype(jnp.float32), 0.0).astype(jnp.bfloat16)
        both = jnp.concatenate([vec, top_only], axis=0)
        total[...] += dot(t_buf[par][...], both, ((1,), (0,)))

    def backward(which, chunk, par):
        full = dot(dt[...], t_buf[par][:, :width], ((1,), (0,)))
        rest = dot(dt[:rhs_n, :], t_buf[par][:, width:], ((1,), (0,)))
        ret_out[which, chunk] = full[:rhs_n] + full[rhs_n:] + rest

    def transposed(total):
        turned = total[...].T
        return turned[:rhs_n] + turned[rhs_n:]

    acc[...] = jnp.zeros_like(acc)
    t1[...] = jnp.zeros_like(t1)
    tiles = 5
    steps = tiles * CHUNKS

    def arrive(step):
        slot = step // CHUNKS
        chunk = lax.rem(step, CHUNKS)

        @pl.when(jnp.logical_and(slot >= 1, slot < tiles))
        def _():
            @pl.when(chunk == 0)
            def _():
                m_copy(OWN, slot, 0, me).wait_recv()

            x_copy(OWN, slot, chunk, 0, me).wait_recv()
            for there in (fwd_m2, fwd_p33):
                way, src, dst, offset = there

                @pl.when(slot == src)
                def _():
                    @pl.when(chunk == 0)
                    def _():
                        m_copy(src, dst, way, at(offset)).start()

                    x_copy(src, dst, chunk, way, at(offset)).start()

    gram(OWN, OWN, 0, 0)

    @pl.loop(0, steps // 2)
    def _(pair):
        arrive(2 * pair + 1)
        arrive(2 * pair + 2)
        for par in (0, 1):
            step = 2 * pair + par
            after = lax.rem(step + 1, steps)
            before = jnp.maximum(step - 1, 0)
            gram(OWN, after // CHUNKS, lax.rem(after, CHUNKS), 1 - par)
            elem(0, step // CHUNKS, lax.rem(step, CHUNKS), par)
            forward(acc, before // CHUNKS, lax.rem(before, CHUNKS), 1 - par)

    forward(acc, tiles - 1, CHUNKS - 1, 1)

    for which, left_slot, slot, back_to, ahead_to in ((0, M2, P1, 1, -2), (1, M32, P33, 33, -32)):
        late = M2 if which == 0 else P33
        m_copy(OWN, late, 0, me).wait_recv()
        for chunk in range(CHUNKS):
            x_copy(OWN, late, chunk, 0, me).wait_recv()
        for r in range(pts // 128):
            half_col[1, r * 128 : (r + 1) * 128, :] = jnp.broadcast_to(
                meta[left_slot, r : r + 1, :], (128, 128)
            ).T
        dt[...] = blk[left_slot, 1].T
        acc2[...] = jnp.zeros_like(acc2)
        gram(left_slot, slot, 0, 0)
        for chunk in range(CHUNKS):
            par = chunk % 2
            if chunk + 1 < CHUNKS:
                gram(left_slot, slot, chunk + 1, 1 - par)
            elem(1, slot, chunk, par)
            if chunk > 0:
                forward(acc2, slot, chunk - 1, 1 - par)
                backward(2 * which, chunk - 1, 1 - par)
        forward(acc2, slot, CHUNKS - 1, (CHUNKS - 1) % 2)
        backward(2 * which, CHUNKS - 1, (CHUNKS - 1) % 2)
        ahead = transposed(acc2)
        for chunk in range(CHUNKS):
            ret_out[2 * which + 1, chunk] = ahead[:, chunk * width : (chunk + 1) * width]
        for kind, offset in ((2 * which, back_to), (2 * which + 1, ahead_to)):
            pltpu.make_async_remote_copy(
                src_ref=ret_out.at[kind],
                dst_ref=ret_in.at[kind],
                send_sem=r_send.at[kind],
                recv_sem=r_recv.at[kind],
                device_id=(at(offset),),
                device_id_type=MESH,
            ).start()

    def ret_copy(kind):
        return pltpu.make_async_remote_copy(
            src_ref=ret_out.at[kind],
            dst_ref=ret_in.at[kind],
            send_sem=r_send.at[kind],
            recv_sem=r_recv.at[kind],
            device_id=(me,),
            device_id_type=MESH,
        )

    own_part = transposed(acc)
    for kind in range(4):
        ret_copy(kind).wait_recv()
    loads[2].wait()
    scale = outputscale[0] * (10.0 / 3.0)
    noise = noise_var[0]
    lane_sums = [jnp.zeros((rhs_n, 128), jnp.float32)] * 4
    for chunk in range(CHUNKS):
        lanes = slice(chunk * width, (chunk + 1) * width)
        there = ret_in[0, chunk] + ret_in[1, chunk] + ret_in[2, chunk] + ret_in[3, chunk]
        vec, old = dvec[:, lanes], res[:, lanes]
        applied = noise * vec + scale * (own_part[:, lanes] + there)
        applied_ref[:, lanes] = applied
        for at_sum, term in enumerate((old * old, vec * applied, old * applied, applied * applied)):
            for h in range(width // 128):
                lane_sums[at_sum] = lane_sums[at_sum] + term[:, h * 128 : (h + 1) * 128]
    rows = [
        jnp.sum(jnp.concatenate(lane_sums[2 * i : 2 * i + 2], axis=0).T, axis=0, keepdims=True)
        for i in range(2)
    ]
    running = jnp.concatenate(rows + [jnp.zeros((6, 128), jnp.float32)], axis=0)

    base = 0
    for stride, size in stages:
        sums[base] = running
        place = lax.rem(me // stride, size)
        copies = []
        for k in range(1, size):
            copies.append(pltpu.make_async_remote_copy(
                src_ref=sums.at[base],
                dst_ref=sums.at[base + k],
                send_sem=a_send.at[base + k],
                recv_sem=a_recv.at[base + k],
                device_id=(group_peer(stride, size, k),),
                device_id_type=MESH,
            ))
        for copy in copies:
            copy.start()
        for copy in copies:
            copy.wait_recv()
        parts = [sums[base + lax.rem(place - member + size, size)] for member in range(size)]
        running = parts[0]
        for part in parts[1:]:
            running = running + part
        base += size

    mean = running * (1.0 / (n_dev * pts))
    swapped = pltpu.roll(mean, 64, 1)
    old_norm, curvature = mean[0:1], swapped[0:1]
    cross_term, applied_norm = mean[1:2], swapped[1:2]
    step_size = old_norm / jnp.maximum(curvature, 1.0)
    updated = old_norm - 2.0 * step_size * cross_term + step_size * step_size * applied_norm
    ratio = updated / (old_norm + 1e-6)
    for i, value in enumerate((step_size, ratio)):
        coef_ref[:, i * 128 : (i + 1) * 128] = jnp.broadcast_to(value, (128, 128)).T[:rhs_n]

    for way, src, dst, offset in own_ways + (fwd_m2, fwd_p33):
        m_copy(src, dst, way, me).wait_send()
        for chunk in range(CHUNKS):
            x_copy(src, dst, chunk, way, me).wait_send()
    for kind in range(4):
        ret_copy(kind).wait_send()
    base = 0
    for stride, size in stages:
        for k in range(1, size):
            pltpu.make_async_remote_copy(
                src_ref=sums.at[base],
                dst_ref=sums.at[base + k],
                send_sem=a_send.at[base + k],
                recv_sem=a_recv.at[base + k],
                device_id=(me,),
                device_id_type=MESH,
            ).wait_send()
        base += size


def local(n_dev, features, lengthscale, noise_var, outputscale, solution, residual, direction):
    pts, feat_n = features.shape
    rhs_n = direction.shape[1]
    width = pts // CHUNKS
    f32, bf16 = jnp.float32, jnp.bfloat16
    dma = pltpu.SemaphoreType.DMA
    in_place = pl.BlockSpec(memory_space=pl.ANY)
    vmem = pl.BlockSpec(memory_space=pltpu.VMEM)
    smem = pl.BlockSpec(memory_space=pltpu.SMEM)
    n_sums = 8 + 4 + n_dev // 32

    def body(*refs):
        kernel(n_dev, width, *refs)

    applied, coef = pl.pallas_call(
        body,
        out_shape=(
            jax.ShapeDtypeStruct((rhs_n, pts), f32),
            jax.ShapeDtypeStruct((rhs_n, 256), f32),
        ),
        in_specs=[in_place, vmem, smem, smem, in_place, in_place],
        out_specs=(vmem, vmem),
        scratch_shapes=[
            pltpu.VMEM((pts, feat_n), bf16),
            pltpu.VMEM((rhs_n, pts), f32),
            pltpu.VMEM((rhs_n, pts), f32),
            pltpu.VMEM((7, 2, pts, 128), bf16),
            pltpu.VMEM((7, 8, 128), f32),
            pltpu.VMEM((2, pts, 128), f32),
            pltpu.VMEM((2 * rhs_n, pts), bf16),
            pltpu.VMEM((pts, width), f32),
            pltpu.VMEM((pts, width), f32),
            pltpu.VMEM((pts, 2 * width), bf16),
            pltpu.VMEM((pts, 2 * width), bf16),
            pltpu.VMEM((2 * width, 128), bf16),
            pltpu.VMEM((pts, 128), f32),
            pltpu.VMEM((pts, 128), f32),
            pltpu.VMEM((4, CHUNKS, rhs_n, width), f32),
            pltpu.VMEM((4, CHUNKS, rhs_n, width), f32),
            pltpu.VMEM((n_sums, 8, 128), f32),
            dma((3,)),
            dma((6, CHUNKS)),
            dma((7, CHUNKS)),
            dma((6,)),
            dma((7,)),
            dma((4,)),
            dma((4,)),
            dma((n_sums,)),
            dma((n_sums,)),
        ],
        compiler_params=pltpu.CompilerParams(
            collective_id=0, has_side_effects=True, vmem_limit_bytes=48 * 1024 * 1024
        ),
        name="cg_step",
    )(features, lengthscale.reshape(1, feat_n), noise_var, outputscale, direction.T, residual.T)
    applied = applied.T
    step_size, ratio = coef[:, 0], coef[:, 128]
    new_solution = solution + step_size[None, :] * direction
    new_residual = residual - step_size[None, :] * applied
    new_direction = new_residual + ratio[None, :] * direction
    return (new_solution, new_residual, new_direction)


def solution(mesh):
    n_dev = mesh.shape[AXIS]
    rows = P(AXIS, None)

    def whole(*arrays):
        return local(n_dev, *arrays)

    return jax.shard_map(
        whole,
        mesh=mesh,
        in_specs=(rows, P(), P(), P(), rows, rows, rows),
        out_specs=(rows, rows, rows),
        check_vma=False,
    )
```

```python
import math

import jax
import jax.numpy as jnp
from jax import lax
from jax.experimental import pallas as pl
from jax.experimental.pallas import tpu as pltpu
from jax.sharding import PartitionSpec as P

AXIS = "blk"
MESH = pl.DeviceIdType.MESH
OWN, P1, M1, P32, M32, M2, P33 = range(7)
CHUNKS = 4
PLANE = 32
SPAN = 120.0
STRIP = 64

RATE = math.sqrt(10.0) * math.log2(math.e)
POLY_P = 3.0 / math.sqrt(10.0)
POLY_Q = 0.3
TINY = 1e-30


def dot(left, right, dims):
    return lax.dot_general(left, right, (dims, ((), ())), preferred_element_type=jnp.float32)


def kernel(
    n_dev, width, features, lengthscale, noise_var, outputscale, direction, residual,
    applied_ref, coef_ref,
    feat, dvec, res, xbuf, dbuf, meta, half_col, dt, s0, s1, t0, t1, acc, acc2, ret_out, ret_in, sums,
    load_sem, x_send, x_recv, d_send, d_recv, m_send, m_recv, r_send, r_recv, a_send, a_recv,
):
    me = lax.axis_index(AXIS)
    pts = width * CHUNKS
    part = width // 2
    rhs_n = direction.shape[0]
    s_buf, t_buf = (s0, s1), (t0, t1)
    in_plane = lax.rem(me, PLANE)

    def at(offset):
        return lax.rem(me + (offset + n_dev), n_dev)

    def group_peer(stride, size, k):
        place = lax.rem(me // stride, size)
        return me + (lax.rem(place + k, size) - place) * stride

    stages = ((1, 8), (8, 4), (32, n_dev // 32))
    loads = [
        pltpu.make_async_copy(features, feat, load_sem.at[0]),
        pltpu.make_async_copy(direction, dvec, load_sem.at[1]),
        pltpu.make_async_copy(residual, res, load_sem.at[2]),
    ]
    for load in loads:
        load.start()

    barrier = pltpu.get_barrier_semaphore()
    peers = [at(o) for o in (1, -1, 2, -2, 32, -32, 33, -33)]
    peers += [group_peer(1, PLANE, k) for k in (1, 2, PLANE - 1, PLANE - 2)]
    for stride, size in stages:
        peers += [group_peer(stride, size, k) for k in range(1, size)]
    for peer in peers:
        pl.semaphore_signal(barrier, inc=1, device_id=(peer,), device_id_type=MESH)

    last = PLANE - 1
    ways = (
        (OWN, P32, -32, None),
        (OWN, M32, 32, None),
        (OWN, P1, -1, in_plane != 0),
        (OWN, M1, 1, in_plane != last),
        (P32, P33, -1, None),
        (M1, M2, 1, in_plane != last),
        (P32, P1, last, in_plane == 0),
        (M32, M1, -last, in_plane == last),
        (M32, M2, 1 - last, in_plane == last - 1),
    )

    def block_copies(way, chunk):
        src, dst, offset, _ = ways[way]
        rows = pl.ds(pl.multiple_of(chunk * width, width), width)
        device = (at(offset),)
        return (
            pltpu.make_async_remote_copy(
                src_ref=xbuf.at[src, rows, :],
                dst_ref=xbuf.at[dst, rows, :],
                send_sem=x_send.at[way, chunk],
                recv_sem=x_recv.at[dst, chunk],
                device_id=device,
                device_id_type=MESH,
            ),
            pltpu.make_async_remote_copy(
                src_ref=dbuf.at[src, chunk],
                dst_ref=dbuf.at[dst, chunk],
                send_sem=d_send.at[way, chunk],
                recv_sem=d_recv.at[dst, chunk],
                device_id=device,
                device_id_type=MESH,
            ),
        )

    def meta_copy(way):
        src, dst, offset, _ = ways[way]
        return pltpu.make_async_remote_copy(
            src_ref=meta.at[src],
            dst_ref=meta.at[dst],
            send_sem=m_send.at[way],
            recv_sem=m_recv.at[dst],
            device_id=(at(offset),),
            device_id_type=MESH,
        )

    def where_sent(way, action):
        if ways[way][3] is None:
            action()
        else:
            pl.when(ways[way][3])(action)

    def send_chunk(way, chunk, with_meta):
        def go():
            if with_meta is True:
                meta_copy(way).start()
            elif with_meta is not False:
                pl.when(with_meta)(lambda: meta_copy(way).start())
            for copy in block_copies(way, chunk):
                copy.start()

        where_sent(way, go)

    first_way = {dst: way for way, (_, dst, _, _) in reversed(list(enumerate(ways)))}

    def got_chunk(slot, chunk):
        for copy in block_copies(first_way[slot], chunk):
            copy.wait_recv()

    def got_meta(slot):
        meta_copy(first_way[slot]).wait_recv()

    def encode(packed):
        most = jnp.maximum(jnp.max(jnp.abs(packed), axis=0, keepdims=True), TINY)
        power = jnp.floor(jnp.log2(SPAN / most))
        times = jnp.exp2(power).astype(jnp.bfloat16).astype(jnp.float32)
        back = jnp.broadcast_to(jnp.exp2(-power), (16, 128))
        return jnp.exp2(packed * times).astype(jnp.bfloat16), back.astype(jnp.bfloat16)

    def decode(ref):
        back = ref[part:, :].astype(jnp.float32)[0:1]
        return jnp.log(ref[:part, :].astype(jnp.float32)) * (back * (1.0 / math.log(2.0)))

    def low_lanes(shape):
        return lax.broadcasted_iota(jnp.int32, shape, 1) < rhs_n

    def vectors(slot, chunk):
        value = decode(dbuf.at[slot, chunk])
        high = value.astype(jnp.bfloat16).astype(jnp.float32)
        low = value - high
        high_r, low_r = pltpu.roll(high, rhs_n, 1), pltpu.roll(low, rhs_n, 1)
        left = low_lanes(value.shape)
        both = jnp.concatenate([jnp.where(left, high, low_r), jnp.where(left, high_r, low)], axis=0)
        top = jnp.concatenate([jnp.where(left, high, 0.0), jnp.where(left, high_r, 0.0)], axis=0)
        return both.astype(jnp.bfloat16), top.astype(jnp.bfloat16)

    def pack_rows(block):
        return jnp.concatenate([block[:, :part], block[:, part:]], axis=0).T

    loads[0].wait()
    scaled = (feat[...].astype(jnp.float32) / lengthscale[...]).astype(jnp.bfloat16)
    xbuf[OWN] = scaled
    exact = scaled.astype(jnp.float32)
    half = 0.5 * jnp.sum(exact * exact, axis=1, keepdims=True)
    half_col[0] = jnp.broadcast_to(half, (pts, 128))
    for r in range(pts // 128):
        meta[OWN, r : r + 1, :] = half_col[0, r * 128 : (r + 1) * 128, :].T[0:1, :]
    loads[1].wait()
    for chunk in range(CHUNKS):
        code, back = encode(pack_rows(dvec[:, chunk * width : (chunk + 1) * width]))
        dbuf[OWN, chunk, :part] = code
        dbuf[OWN, chunk, part:] = back

    pl.semaphore_wait(barrier, len(peers))
    for chunk in range(CHUNKS):
        for way in range(4):
            send_chunk(way, chunk, chunk == 0)

    def gram(left_slot, slot, chunk, par):
        rows = pl.ds(pl.multiple_of(chunk * width, width), width)
        s_buf[par][...] = dot(xbuf[left_slot], xbuf[slot, rows, :], ((1,), (1,)))

    def elem(half_slot, slot, chunk, par):
        for h in range(width // 128):
            row = meta[slot, pl.ds(chunk * (width // 128) + h, 1), :]
            for strip in range(pts // STRIP):
                rows = slice(strip * STRIP, (strip + 1) * STRIP)
                lanes = slice(h * 128, (h + 1) * 128)
                u = (half_col[half_slot, rows, :] + row) - s_buf[par][rows, lanes]
                u = jnp.maximum(u, TINY)
                r = u * lax.rsqrt(u)
                value = ((r + POLY_P) * r + POLY_Q) * jnp.exp2(r * (-RATE))
                top = value.astype(jnp.bfloat16)
                rest = (value - top.astype(jnp.float32)).astype(jnp.bfloat16)
                t_buf[par][rows, lanes] = top
                t_buf[par][rows, slice(width + h * 128, width + (h + 1) * 128)] = rest

    def forward(total, slot, chunk, par):
        both, top = vectors(slot, chunk)
        total[...] += dot(t_buf[par][...], jnp.concatenate([both, top], axis=0), ((1,), (0,)))

    def backward(kind, chunk, par):
        full = dot(dt[...], t_buf[par][:, :width], ((1,), (0,)))
        rest = dot(dt[:rhs_n, :], t_buf[par][:, width:], ((1,), (0,)))
        code, back = encode(pack_rows(full[:rhs_n] + full[rhs_n:] + rest))
        ret_out[kind, chunk, :part] = code
        ret_out[kind, chunk, part:] = back

    def ret_copy(kind, chunk, offset=1):
        return pltpu.make_async_remote_copy(
            src_ref=ret_out.at[kind, chunk],
            dst_ref=ret_in.at[kind, chunk],
            send_sem=r_send.at[kind, chunk],
            recv_sem=r_recv.at[kind, chunk],
            device_id=(at(offset),),
            device_id_type=MESH,
        )

    def transposed(total):
        turned = total[...].T
        return turned[:rhs_n] + turned[rhs_n:]

    def run(left_slot, half_slot, steps, place, total, each_pair=None, kind=None):
        t1[...] = jnp.zeros_like(t1)
        gram(left_slot, *place(0), 0)

        @pl.loop(0, steps // 2)
        def _(pair):
            if each_pair is not None:
                each_pair(pair)
            for par in (0, 1):
                step = 2 * pair + par
                gram(left_slot, *place(lax.rem(step + 1, steps)), 1 - par)
                elem(half_slot, *place(step), par)
                before = place(jnp.maximum(step - 1, 0))
                forward(total, *before, 1 - par)
                if kind is not None:
                    backward(kind, before[1], 1 - par)

        final = place(steps - 1)
        forward(total, *final, 1)
        if kind is not None:
            backward(kind, final[1], 1)

    acc[...] = jnp.zeros_like(acc)

    def first_place(step):
        later = (step - CHUNKS) // 2
        if isinstance(step, int):
            return (OWN, step) if step < CHUNKS else (P32 + step % 2, later)
        own = step < CHUNKS
        return jnp.where(own, OWN, P32 + lax.rem(step, 2)), jnp.where(own, step, later)

    def pass_on(slot, chunk, with_meta):
        got_chunk(slot, chunk)
        for way, (src, _, _, _) in enumerate(ways):
            if src == slot:
                send_chunk(way, chunk, with_meta)

    def first_arrivals(pair):
        for slot, lag in ((P32, 1), (M32, 2), (M1, 3)):
            chunk = pair - lag

            @pl.when(jnp.logical_and(chunk >= 0, chunk < CHUNKS))
            def _():
                pl.when(chunk == 0)(lambda: got_meta(slot))
                pass_on(slot, chunk, chunk == 0)

    run(OWN, 0, 3 * CHUNKS, first_place, acc, first_arrivals)
    pass_on(M1, CHUNKS - 1, False)

    for kind, left_slot, slot, back_to, ahead_to in ((0, M32, P33, 33, -32), (2, M2, P1, 1, -2)):
        for late in (P33,) if kind == 0 else (M2, P1):
            got_meta(late)
            for chunk in range(CHUNKS):
                got_chunk(late, chunk)
        for r in range(pts // 128):
            half_col[1, r * 128 : (r + 1) * 128, :] = jnp.broadcast_to(
                meta[left_slot, r : r + 1, :], (128, 128)
            ).T
        for chunk in range(CHUNKS):
            dt[:, chunk * width : (chunk + 1) * width] = vectors(left_slot, chunk)[0].T
        acc2[...] = jnp.zeros_like(acc2)
        run(left_slot, 1, CHUNKS, lambda step, slot=slot: (slot, step), acc2, None, kind)
        for chunk in range(CHUNKS):
            ahead = acc2[chunk * width : (chunk + 1) * width, :]
            ahead = ahead + pltpu.roll(ahead, rhs_n, 1)
            ahead = jnp.where(low_lanes((part, 128)), ahead[:part], ahead[part:])
            code, back = encode(ahead)
            ret_out[kind + 1, chunk, :part] = code
            ret_out[kind + 1, chunk, part:] = back
            ret_copy(kind, chunk, back_to).start()
            ret_copy(kind + 1, chunk, ahead_to).start()

    def last_place(step):
        return step // CHUNKS + P1, step % CHUNKS if isinstance(step, int) else lax.rem(step, CHUNKS)

    run(OWN, 0, 2 * CHUNKS, last_place, acc)

    for kind in range(4):
        for chunk in range(CHUNKS):
            ret_copy(kind, chunk).wait_recv()
    for chunk in range(CHUNKS):
        there = decode(ret_in.at[0, chunk])
        for kind in range(1, 4):
            there = there + decode(ret_in.at[kind, chunk])
        left = low_lanes(there.shape)
        acc[chunk * width : chunk * width + part, :] += jnp.where(left, there, 0.0)
        acc[chunk * width + part : (chunk + 1) * width, :] += jnp.where(left, 0.0, there)
    own_part = transposed(acc)
    loads[2].wait()
    scale = outputscale[0] * (10.0 / 3.0)
    noise = noise_var[0]
    lane_sums = [jnp.zeros((rhs_n, 128), jnp.float32)] * 4
    for chunk in range(CHUNKS):
        lanes = slice(chunk * width, (chunk + 1) * width)
        vec, old = dvec[:, lanes], res[:, lanes]
        applied = noise * vec + scale * own_part[:, lanes]
        applied_ref[:, lanes] = applied
        for at_sum, term in enumerate((old * old, vec * applied, old * applied, applied * applied)):
            for h in range(width // 128):
                lane_sums[at_sum] = lane_sums[at_sum] + term[:, h * 128 : (h + 1) * 128]
    rows = [
        jnp.sum(jnp.concatenate(lane_sums[2 * i : 2 * i + 2], axis=0).T, axis=0, keepdims=True)
        for i in range(2)
    ]
    running = jnp.concatenate(rows + [jnp.zeros((6, 128), jnp.float32)], axis=0)

    base = 0
    for stride, size in stages:
        sums[base] = running
        place = lax.rem(me // stride, size)
        copies = []
        for k in range(1, size):
            copies.append(pltpu.make_async_remote_copy(
                src_ref=sums.at[base],
                dst_ref=sums.at[base + k],
                send_sem=a_send.at[base + k],
                recv_sem=a_recv.at[base + k],
                device_id=(group_peer(stride, size, k),),
                device_id_type=MESH,
            ))
        for copy in copies:
            copy.start()
        for copy in copies:
            copy.wait_recv()
        parts = [sums[base + lax.rem(place - member + size, size)] for member in range(size)]
        running = parts[0]
        for part in parts[1:]:
            running = running + part
        base += size

    mean = running * (1.0 / (n_dev * pts))
    swapped = pltpu.roll(mean, 64, 1)
    old_norm, curvature = mean[0:1], swapped[0:1]
    cross_term, applied_norm = mean[1:2], swapped[1:2]
    step_size = old_norm / jnp.maximum(curvature, 1.0)
    updated = old_norm - 2.0 * step_size * cross_term + step_size * step_size * applied_norm
    ratio = updated / (old_norm + 1e-6)
    for i, value in enumerate((step_size, ratio)):
        coef_ref[:, i * 128 : (i + 1) * 128] = jnp.broadcast_to(value, (128, 128)).T[:rhs_n]

    for way in range(len(ways)):
        def left(way=way):
            meta_copy(way).wait_send()
            for chunk in range(CHUNKS):
                for copy in block_copies(way, chunk):
                    copy.wait_send()

        where_sent(way, left)
    for kind in range(4):
        for chunk in range(CHUNKS):
            ret_copy(kind, chunk).wait_send()
    base = 0
    for stride, size in stages:
        for k in range(1, size):
            pltpu.make_async_remote_copy(
                src_ref=sums.at[base],
                dst_ref=sums.at[base + k],
                send_sem=a_send.at[base + k],
                recv_sem=a_recv.at[base + k],
                device_id=(me,),
                device_id_type=MESH,
            ).wait_send()
        base += size


def local(n_dev, features, lengthscale, noise_var, outputscale, solution, residual, direction):
    pts, feat_n = features.shape
    rhs_n = direction.shape[1]
    width = pts // CHUNKS
    f32, bf16 = jnp.float32, jnp.bfloat16
    dma = pltpu.SemaphoreType.DMA
    in_place = pl.BlockSpec(memory_space=pltpu.HBM)
    vmem = pl.BlockSpec(memory_space=pltpu.VMEM)
    smem = pl.BlockSpec(memory_space=pltpu.SMEM)
    n_sums = 8 + 4 + n_dev // 32

    def body(*refs):
        kernel(n_dev, width, *refs)

    applied, coef = pl.pallas_call(
        body,
        out_shape=(
            jax.ShapeDtypeStruct((rhs_n, pts), f32),
            jax.ShapeDtypeStruct((rhs_n, 256), f32),
        ),
        in_specs=[in_place, vmem, smem, smem, in_place, in_place],
        out_specs=(vmem, vmem),
        scratch_shapes=[
            pltpu.VMEM((pts, feat_n), bf16),
            pltpu.VMEM((rhs_n, pts), f32),
            pltpu.VMEM((rhs_n, pts), f32),
            pltpu.VMEM((7, pts, feat_n), bf16),
            pltpu.VMEM((7, CHUNKS, width // 2 + 16, 128), bf16),
            pltpu.VMEM((7, 8, 128), f32),
            pltpu.VMEM((2, pts, 128), f32),
            pltpu.VMEM((2 * rhs_n, pts), bf16),
            pltpu.VMEM((pts, width), f32),
            pltpu.VMEM((pts, width), f32),
            pltpu.VMEM((pts, 2 * width), bf16),
            pltpu.VMEM((pts, 2 * width), bf16),
            pltpu.VMEM((pts, 128), f32),
            pltpu.VMEM((pts, 128), f32),
            pltpu.VMEM((4, CHUNKS, width // 2 + 16, 128), bf16),
            pltpu.VMEM((4, CHUNKS, width // 2 + 16, 128), bf16),
            pltpu.VMEM((n_sums, 8, 128), f32),
            dma((3,)),
            dma((9, CHUNKS)),
            dma((7, CHUNKS)),
            dma((9, CHUNKS)),
            dma((7, CHUNKS)),
            dma((9,)),
            dma((7,)),
            dma((4, CHUNKS)),
            dma((4, CHUNKS)),
            dma((n_sums,)),
            dma((n_sums,)),
        ],
        compiler_params=pltpu.CompilerParams(
            collective_id=0, has_side_effects=True, vmem_limit_bytes=60 * 1024 * 1024
        ),
        name="cg_step",
    )(features, lengthscale.reshape(1, feat_n), noise_var, outputscale, direction.T, residual.T)
    applied = applied.T
    step_size, ratio = coef[:, 0], coef[:, 128]
    new_solution = solution + step_size[None, :] * direction
    new_residual = residual - step_size[None, :] * applied
    new_direction = new_residual + ratio[None, :] * direction
    return (new_solution, new_residual, new_direction)


def solution(mesh):
    n_dev = mesh.shape[AXIS]
    rows = P(AXIS, None)

    def whole(*arrays):
        return local(n_dev, *arrays)

    return jax.shard_map(
        whole,
        mesh=mesh,
        in_specs=(rows, P(), P(), P(), rows, rows, rows),
        out_specs=(rows, rows, rows),
        check_vma=False,
    )
```

```python
import math

import jax
import jax.numpy as jnp
from jax import lax
from jax.experimental import pallas as pl
from jax.experimental.pallas import tpu as pltpu
from jax.sharding import PartitionSpec as P

AXIS = "blk"
MESH = pl.DeviceIdType.MESH
OWN, P1, M1, P32, M32, M2, P33 = range(7)
CHUNKS = 4
PLANE = 32
SPAN = 120.0
STRIP = 64

RATE = math.sqrt(10.0) * math.log2(math.e)
POLY_P = 3.0 / math.sqrt(10.0)
POLY_Q = 0.3
TINY = 1e-30


def dot(left, right, dims):
    return lax.dot_general(left, right, (dims, ((), ())), preferred_element_type=jnp.float32)


def kernel(
    n_dev, width, features, lengthscale, noise_var, outputscale, direction, residual,
    applied_ref, coef_ref,
    feat, dvec, res, xbuf, dbuf, meta, half_col, dt, s0, s1, t0, t1, middle, centre, dsum, acc, acc2, ret_out, ret_in, sums,
    load_sem, x_send, x_recv, d_send, d_recv, m_send, m_recv, r_send, r_recv, a_send, a_recv,
):
    me = lax.axis_index(AXIS)
    pts = width * CHUNKS
    part = width // 2
    rhs_n = direction.shape[0]
    s_buf, t_buf = (s0, s1), (t0, t1)
    in_plane = lax.rem(me, PLANE)

    def at(offset):
        return lax.rem(me + (offset + n_dev), n_dev)

    def group_peer(stride, size, k):
        place = lax.rem(me // stride, size)
        return me + (lax.rem(place + k, size) - place) * stride

    stages = ((1, 8), (8, 4), (32, n_dev // 32))
    loads = [
        pltpu.make_async_copy(features, feat, load_sem.at[0]),
        pltpu.make_async_copy(direction, dvec, load_sem.at[1]),
        pltpu.make_async_copy(residual, res, load_sem.at[2]),
    ]
    for load in loads:
        load.start()

    barrier = pltpu.get_barrier_semaphore()
    peers = [at(o) for o in (1, -1, 2, -2, 32, -32, 33, -33)]
    peers += [group_peer(1, PLANE, k) for k in (1, 2, PLANE - 1, PLANE - 2)]
    for stride, size in stages:
        peers += [group_peer(stride, size, k) for k in range(1, size)]
    for peer in peers:
        pl.semaphore_signal(barrier, inc=1, device_id=(peer,), device_id_type=MESH)

    last = PLANE - 1
    ways = (
        (OWN, P32, -32, None),
        (OWN, M32, 32, None),
        (OWN, P1, -1, in_plane != 0),
        (OWN, M1, 1, in_plane != last),
        (P32, P33, -1, None),
        (M1, M2, 1, in_plane != last),
        (P32, P1, last, in_plane == 0),
        (M32, M1, -last, in_plane == last),
        (M32, M2, 1 - last, in_plane == last - 1),
    )

    def block_copies(way, chunk):
        src, dst, offset, _ = ways[way]
        rows = pl.ds(pl.multiple_of(chunk * width, width), width)
        device = (at(offset),)
        return (
            pltpu.make_async_remote_copy(
                src_ref=xbuf.at[src, rows, :],
                dst_ref=xbuf.at[dst, rows, :],
                send_sem=x_send.at[way, chunk],
                recv_sem=x_recv.at[dst, chunk],
                device_id=device,
                device_id_type=MESH,
            ),
            pltpu.make_async_remote_copy(
                src_ref=dbuf.at[src, chunk],
                dst_ref=dbuf.at[dst, chunk],
                send_sem=d_send.at[way, chunk],
                recv_sem=d_recv.at[dst, chunk],
                device_id=device,
                device_id_type=MESH,
            ),
        )

    def meta_copy(way):
        src, dst, offset, _ = ways[way]
        return pltpu.make_async_remote_copy(
            src_ref=meta.at[src],
            dst_ref=meta.at[dst],
            send_sem=m_send.at[way],
            recv_sem=m_recv.at[dst],
            device_id=(at(offset),),
            device_id_type=MESH,
        )

    def where_sent(way, action):
        if ways[way][3] is None:
            action()
        else:
            pl.when(ways[way][3])(action)

    def send_chunk(way, chunk, with_meta):
        def go():
            if with_meta is True:
                meta_copy(way).start()
            elif with_meta is not False:
                pl.when(with_meta)(lambda: meta_copy(way).start())
            for copy in block_copies(way, chunk):
                copy.start()

        where_sent(way, go)

    first_way = {dst: way for way, (_, dst, _, _) in reversed(list(enumerate(ways)))}

    def got_chunk(slot, chunk):
        for copy in block_copies(first_way[slot], chunk):
            copy.wait_recv()

    def got_meta(slot):
        meta_copy(first_way[slot]).wait_recv()

    def encode(packed):
        most = jnp.maximum(jnp.max(jnp.abs(packed), axis=0, keepdims=True), TINY)
        power = jnp.floor(jnp.log2(SPAN / most))
        times = jnp.exp2(power).astype(jnp.bfloat16).astype(jnp.float32)
        back = jnp.broadcast_to(jnp.exp2(-power), (16, 128))
        return jnp.exp2(packed * times).astype(jnp.bfloat16), back.astype(jnp.bfloat16)

    def decode(ref):
        back = ref[part:, :].astype(jnp.float32)[0:1]
        return jnp.log(ref[:part, :].astype(jnp.float32)) * (back * (1.0 / math.log(2.0)))

    def low_lanes(shape):
        return lax.broadcasted_iota(jnp.int32, shape, 1) < rhs_n

    def vectors(slot, chunk):
        value = decode(dbuf.at[slot, chunk])
        high = value.astype(jnp.bfloat16).astype(jnp.float32)
        low = value - high
        high_r, low_r = pltpu.roll(high, rhs_n, 1), pltpu.roll(low, rhs_n, 1)
        left = low_lanes(value.shape)
        both = jnp.concatenate([jnp.where(left, high, low_r), jnp.where(left, high_r, low)], axis=0)
        top = jnp.concatenate([jnp.where(left, high, 0.0), jnp.where(left, high_r, 0.0)], axis=0)
        return both.astype(jnp.bfloat16), top.astype(jnp.bfloat16)

    def pack_rows(block):
        return jnp.concatenate([block[:, :part], block[:, part:]], axis=0).T

    loads[0].wait()
    scaled = (feat[...].astype(jnp.float32) / lengthscale[...]).astype(jnp.bfloat16)
    xbuf[OWN] = scaled
    exact = scaled.astype(jnp.float32)
    half = 0.5 * jnp.sum(exact * exact, axis=1, keepdims=True)
    half_col[0] = jnp.broadcast_to(half, (pts, 128))
    middle[0] = jnp.mean(half_col[0], axis=0, keepdims=True)
    for r in range(pts // 128):
        meta[OWN, r : r + 1, :] = half_col[0, r * 128 : (r + 1) * 128, :].T[0:1, :]
    loads[1].wait()
    for chunk in range(CHUNKS):
        code, back = encode(pack_rows(dvec[:, chunk * width : (chunk + 1) * width]))
        dbuf[OWN, chunk, :part] = code
        dbuf[OWN, chunk, part:] = back

    pl.semaphore_wait(barrier, len(peers))
    for chunk in range(CHUNKS):
        for way in range(4):
            send_chunk(way, chunk, chunk == 0)

    def gram(left_slot, slot, chunk, par):
        rows = pl.ds(pl.multiple_of(chunk * width, width), width)
        s_buf[par][...] = dot(xbuf[left_slot], xbuf[slot, rows, :], ((1,), (1,)))

    def covariance(u):
        r = u * lax.rsqrt(u)
        return ((r + POLY_P) * r + POLY_Q) * jnp.exp2(r * (-RATE))

    def elem(half_slot, slot, chunk, par):
        for h in range(width // 128):
            row = meta[slot, pl.ds(chunk * (width // 128) + h, 1), :]
            mid = covariance(jnp.maximum(middle[half_slot] + row, TINY))
            centre[par, h : h + 1, :] = mid
            for strip in range(pts // STRIP):
                rows = slice(strip * STRIP, (strip + 1) * STRIP)
                lanes = slice(h * 128, (h + 1) * 128)
                u = (half_col[half_slot, rows, :] + row) - s_buf[par][rows, lanes]
                t_buf[par][rows, lanes] = (covariance(jnp.maximum(u, TINY)) - mid).astype(jnp.bfloat16)

    def forward(total, slot, chunk, par):
        both, top = vectors(slot, chunk)
        mid = jnp.concatenate([centre[par, h : h + 1, :] for h in range(width // 128)], axis=1)
        mid = jnp.broadcast_to(mid, (16, width))
        high = mid.astype(jnp.bfloat16)
        low = (mid - high.astype(jnp.float32)).astype(jnp.bfloat16)
        added = dot(high, both, ((1,), (0,))) + dot(low, top, ((1,), (0,)))
        total[...] += dot(t_buf[par][...], both, ((1,), (0,))) + added[0:1]

    def backward(kind, chunk, par):
        full = dot(dt[...], t_buf[par][...], ((1,), (0,)))
        added = [dsum[...] * centre[par, h : h + 1, :] for h in range(width // 128)]
        code, back = encode(pack_rows(full[:rhs_n] + full[rhs_n:] + jnp.concatenate(added, axis=1)))
        ret_out[kind, chunk, :part] = code
        ret_out[kind, chunk, part:] = back

    def ret_copy(kind, chunk, offset=1):
        return pltpu.make_async_remote_copy(
            src_ref=ret_out.at[kind, chunk],
            dst_ref=ret_in.at[kind, chunk],
            send_sem=r_send.at[kind, chunk],
            recv_sem=r_recv.at[kind, chunk],
            device_id=(at(offset),),
            device_id_type=MESH,
        )

    def transposed(total):
        turned = total[...].T
        return turned[:rhs_n] + turned[rhs_n:]

    def run(left_slot, half_slot, steps, place, total, each_pair=None, kind=None):
        t1[...] = jnp.zeros_like(t1)
        centre[1] = jnp.zeros_like(centre[1])
        gram(left_slot, *place(0), 0)

        @pl.loop(0, steps // 2)
        def _(pair):
            if each_pair is not None:
                each_pair(pair)
            for par in (0, 1):
                step = 2 * pair + par
                gram(left_slot, *place(lax.rem(step + 1, steps)), 1 - par)
                elem(half_slot, *place(step), par)
                before = place(jnp.maximum(step - 1, 0))
                forward(total, *before, 1 - par)
                if kind is not None:
                    backward(kind, before[1], 1 - par)

        final = place(steps - 1)
        forward(total, *final, 1)
        if kind is not None:
            backward(kind, final[1], 1)

    acc[...] = jnp.zeros_like(acc)

    def first_place(step):
        later = (step - CHUNKS) // 2
        if isinstance(step, int):
            return (OWN, step) if step < CHUNKS else (P32 + step % 2, later)
        own = step < CHUNKS
        return jnp.where(own, OWN, P32 + lax.rem(step, 2)), jnp.where(own, step, later)

    def pass_on(slot, chunk, with_meta):
        got_chunk(slot, chunk)
        for way, (src, _, _, _) in enumerate(ways):
            if src == slot:
                send_chunk(way, chunk, with_meta)

    def first_arrivals(pair):
        for slot, lag in ((P32, 1), (M32, 2), (M1, 3)):
            chunk = pair - lag

            @pl.when(jnp.logical_and(chunk >= 0, chunk < CHUNKS))
            def _():
                pl.when(chunk == 0)(lambda: got_meta(slot))
                pass_on(slot, chunk, chunk == 0)

    run(OWN, 0, 3 * CHUNKS, first_place, acc, first_arrivals)
    pass_on(M1, CHUNKS - 1, False)

    for kind, left_slot, slot, back_to, ahead_to in ((2, M2, P1, 1, -2), (0, M32, P33, 33, -32)):
        for late in (P33,) if kind == 0 else (M2, P1):
            got_meta(late)
            for chunk in range(CHUNKS):
                got_chunk(late, chunk)
        for r in range(pts // 128):
            half_col[1, r * 128 : (r + 1) * 128, :] = jnp.broadcast_to(
                meta[left_slot, r : r + 1, :], (128, 128)
            ).T
        for chunk in range(CHUNKS):
            dt[:, chunk * width : (chunk + 1) * width] = vectors(left_slot, chunk)[0].T
        middle[1] = jnp.mean(half_col[1], axis=0, keepdims=True)
        total_d = jnp.sum(dt[...].astype(jnp.float32), axis=1, keepdims=True)
        dsum[...] = jnp.broadcast_to(total_d[:rhs_n] + total_d[rhs_n:], (rhs_n, 128))
        acc2[...] = jnp.zeros_like(acc2)
        run(left_slot, 1, CHUNKS, lambda step, slot=slot: (slot, step), acc2, None, kind)
        for chunk in range(CHUNKS):
            ahead = acc2[chunk * width : (chunk + 1) * width, :]
            ahead = ahead + pltpu.roll(ahead, rhs_n, 1)
            ahead = jnp.where(low_lanes((part, 128)), ahead[:part], ahead[part:])
            code, back = encode(ahead)
            ret_out[kind + 1, chunk, :part] = code
            ret_out[kind + 1, chunk, part:] = back
            ret_copy(kind, chunk, back_to).start()
            ret_copy(kind + 1, chunk, ahead_to).start()

    def last_place(step):
        return step // CHUNKS + P1, step % CHUNKS if isinstance(step, int) else lax.rem(step, CHUNKS)

    run(OWN, 0, 2 * CHUNKS, last_place, acc)

    for kind in range(4):
        for chunk in range(CHUNKS):
            ret_copy(kind, chunk).wait_recv()
    for chunk in range(CHUNKS):
        there = decode(ret_in.at[0, chunk])
        for kind in range(1, 4):
            there = there + decode(ret_in.at[kind, chunk])
        left = low_lanes(there.shape)
        acc[chunk * width : chunk * width + part, :] += jnp.where(left, there, 0.0)
        acc[chunk * width + part : (chunk + 1) * width, :] += jnp.where(left, 0.0, there)
    own_part = transposed(acc)
    loads[2].wait()
    scale = outputscale[0] * (10.0 / 3.0)
    noise = noise_var[0]
    lane_sums = [jnp.zeros((rhs_n, 128), jnp.float32)] * 4
    for chunk in range(CHUNKS):
        lanes = slice(chunk * width, (chunk + 1) * width)
        vec, old = dvec[:, lanes], res[:, lanes]
        applied = noise * vec + scale * own_part[:, lanes]
        applied_ref[:, lanes] = applied
        for at_sum, term in enumerate((old * old, vec * applied, old * applied, applied * applied)):
            for h in range(width // 128):
                lane_sums[at_sum] = lane_sums[at_sum] + term[:, h * 128 : (h + 1) * 128]
    rows = [
        jnp.sum(jnp.concatenate(lane_sums[2 * i : 2 * i + 2], axis=0).T, axis=0, keepdims=True)
        for i in range(2)
    ]
    running = jnp.concatenate(rows + [jnp.zeros((6, 128), jnp.float32)], axis=0)

    base = 0
    for stride, size in stages:
        sums[base] = running
        place = lax.rem(me // stride, size)
        copies = []
        for k in range(1, size):
            copies.append(pltpu.make_async_remote_copy(
                src_ref=sums.at[base],
                dst_ref=sums.at[base + k],
                send_sem=a_send.at[base + k],
                recv_sem=a_recv.at[base + k],
                device_id=(group_peer(stride, size, k),),
                device_id_type=MESH,
            ))
        for copy in copies:
            copy.start()
        for copy in copies:
            copy.wait_recv()
        parts = [sums[base + lax.rem(place - member + size, size)] for member in range(size)]
        running = parts[0]
        for part in parts[1:]:
            running = running + part
        base += size

    mean = running * (1.0 / (n_dev * pts))
    swapped = pltpu.roll(mean, 64, 1)
    old_norm, curvature = mean[0:1], swapped[0:1]
    cross_term, applied_norm = mean[1:2], swapped[1:2]
    step_size = old_norm / jnp.maximum(curvature, 1.0)
    updated = old_norm - 2.0 * step_size * cross_term + step_size * step_size * applied_norm
    ratio = updated / (old_norm + 1e-6)
    coef_ref[...] = jnp.concatenate([step_size, ratio, jnp.zeros((6, 128), jnp.float32)], axis=0)

    for way in range(len(ways)):
        def left(way=way):
            meta_copy(way).wait_send()
            for chunk in range(CHUNKS):
                for copy in block_copies(way, chunk):
                    copy.wait_send()

        where_sent(way, left)
    for kind in range(4):
        for chunk in range(CHUNKS):
            ret_copy(kind, chunk).wait_send()
    base = 0
    for stride, size in stages:
        for k in range(1, size):
            pltpu.make_async_remote_copy(
                src_ref=sums.at[base],
                dst_ref=sums.at[base + k],
                send_sem=a_send.at[base + k],
                recv_sem=a_recv.at[base + k],
                device_id=(me,),
                device_id_type=MESH,
            ).wait_send()
        base += size


def local(n_dev, features, lengthscale, noise_var, outputscale, solution, residual, direction):
    pts, feat_n = features.shape
    rhs_n = direction.shape[1]
    width = pts // CHUNKS
    f32, bf16 = jnp.float32, jnp.bfloat16
    dma = pltpu.SemaphoreType.DMA
    in_place = pl.BlockSpec(memory_space=pltpu.HBM)
    vmem = pl.BlockSpec(memory_space=pltpu.VMEM)
    smem = pl.BlockSpec(memory_space=pltpu.SMEM)
    n_sums = 8 + 4 + n_dev // 32

    def body(*refs):
        kernel(n_dev, width, *refs)

    applied, coef = pl.pallas_call(
        body,
        out_shape=(
            jax.ShapeDtypeStruct((rhs_n, pts), f32),
            jax.ShapeDtypeStruct((8, 128), f32),
        ),
        in_specs=[in_place, vmem, smem, smem, in_place, in_place],
        out_specs=(vmem, vmem),
        scratch_shapes=[
            pltpu.VMEM((pts, feat_n), bf16),
            pltpu.VMEM((rhs_n, pts), f32),
            pltpu.VMEM((rhs_n, pts), f32),
            pltpu.VMEM((7, pts, feat_n), bf16),
            pltpu.VMEM((7, CHUNKS, width // 2 + 16, 128), bf16),
            pltpu.VMEM((7, 8, 128), f32),
            pltpu.VMEM((2, pts, 128), f32),
            pltpu.VMEM((2 * rhs_n, pts), bf16),
            pltpu.VMEM((pts, width), f32),
            pltpu.VMEM((pts, width), f32),
            pltpu.VMEM((pts, width), bf16),
            pltpu.VMEM((pts, width), bf16),
            pltpu.VMEM((2, 1, 128), f32),
            pltpu.VMEM((2, width // 128, 128), f32),
            pltpu.VMEM((rhs_n, 128), f32),
            pltpu.VMEM((pts, 128), f32),
            pltpu.VMEM((pts, 128), f32),
            pltpu.VMEM((4, CHUNKS, width // 2 + 16, 128), bf16),
            pltpu.VMEM((4, CHUNKS, width // 2 + 16, 128), bf16),
            pltpu.VMEM((n_sums, 8, 128), f32),
            dma((3,)),
            dma((9, CHUNKS)),
            dma((7, CHUNKS)),
            dma((9, CHUNKS)),
            dma((7, CHUNKS)),
            dma((9,)),
            dma((7,)),
            dma((4, CHUNKS)),
            dma((4, CHUNKS)),
            dma((n_sums,)),
            dma((n_sums,)),
        ],
        compiler_params=pltpu.CompilerParams(
            collective_id=0, has_side_effects=True, vmem_limit_bytes=60 * 1024 * 1024
        ),
        name="cg_step",
    )(features, lengthscale.reshape(1, feat_n), noise_var, outputscale, direction.T, residual.T)
    applied = applied.T
    step_size, ratio = coef[0, :rhs_n], coef[1, :rhs_n]
    new_solution = solution + step_size[None, :] * direction
    new_residual = residual - step_size[None, :] * applied
    new_direction = new_residual + ratio[None, :] * direction
    return (new_solution, new_residual, new_direction)


def solution(mesh):
    n_dev = mesh.shape[AXIS]
    rows = P(AXIS, None)

    def whole(*arrays):
        return local(n_dev, *arrays)

    return jax.shard_map(
        whole,
        mesh=mesh,
        in_specs=(rows, P(), P(), P(), rows, rows, rows),
        out_specs=(rows, rows, rows),
        check_vma=False,
    )
```

```python
import math

import jax
import jax.numpy as jnp
from jax import lax
from jax.experimental import pallas as pl
from jax.experimental.pallas import tpu as pltpu
from jax.sharding import PartitionSpec as P

AXIS = "blk"
MESH = pl.DeviceIdType.MESH
OWN, P1, M1, P32, M32, M2, P33 = range(7)
CHUNKS = 4
PLANE = 32
SPAN = 120.0
STRIP = 64

RATE = math.sqrt(10.0) * math.log2(math.e)
POLY_P = 3.0 / math.sqrt(10.0)
POLY_Q = 0.3
TINY = 1e-30


def dot(left, right, dims):
    return lax.dot_general(left, right, (dims, ((), ())), preferred_element_type=jnp.float32)


def kernel(
    n_dev, width, features, lengthscale, noise_var, outputscale, direction, residual,
    applied_ref, coef_ref,
    feat, dvec, res, xbuf, dbuf, meta, half_col, dt, s0, s1, t0, t1, middle, centre, dsum, acc, acc2, ret_out, ret_in, sums,
    load_sem, x_send, x_recv, d_send, d_recv, m_send, m_recv, r_send, r_recv, a_send, a_recv,
):
    me = lax.axis_index(AXIS)
    pts = width * CHUNKS
    part = width // 2
    rhs_n = direction.shape[0]
    s_buf, t_buf = (s0, s1), (t0, t1)
    in_plane = lax.rem(me, PLANE)

    def at(offset):
        return lax.rem(me + (offset + n_dev), n_dev)

    def group_peer(stride, size, k):
        place = lax.rem(me // stride, size)
        return me + (lax.rem(place + k, size) - place) * stride

    stages = ((1, 8), (8, 4), (32, n_dev // 32))
    loads = [
        pltpu.make_async_copy(features, feat, load_sem.at[0]),
        pltpu.make_async_copy(direction, dvec, load_sem.at[1]),
        pltpu.make_async_copy(residual, res, load_sem.at[2]),
    ]
    for load in loads:
        load.start()

    barrier = pltpu.get_barrier_semaphore()
    peers = [at(o) for o in (1, -1, 2, -2, 32, -32, 33, -33)]
    peers += [group_peer(1, PLANE, k) for k in (1, 2, PLANE - 1, PLANE - 2)]
    for stride, size in stages:
        peers += [group_peer(stride, size, k) for k in range(1, size)]
    for peer in peers:
        pl.semaphore_signal(barrier, inc=1, device_id=(peer,), device_id_type=MESH)

    last = PLANE - 1
    ways = (
        (OWN, P32, -32, None),
        (OWN, M32, 32, None),
        (OWN, P1, -1, in_plane != 0),
        (OWN, M1, 1, in_plane != last),
        (P32, P33, -1, None),
        (M1, M2, 1, in_plane != last),
        (P32, P1, last, in_plane == 0),
        (M32, M1, -last, in_plane == last),
        (M32, M2, 1 - last, in_plane == last - 1),
    )

    def block_copies(way, chunk):
        src, dst, offset, _ = ways[way]
        rows = pl.ds(pl.multiple_of(chunk * width, width), width)
        device = (at(offset),)
        return (
            pltpu.make_async_remote_copy(
                src_ref=xbuf.at[src, rows, :],
                dst_ref=xbuf.at[dst, rows, :],
                send_sem=x_send.at[way, chunk],
                recv_sem=x_recv.at[dst, chunk],
                device_id=device,
                device_id_type=MESH,
            ),
            pltpu.make_async_remote_copy(
                src_ref=dbuf.at[src, chunk],
                dst_ref=dbuf.at[dst, chunk],
                send_sem=d_send.at[way, chunk],
                recv_sem=d_recv.at[dst, chunk],
                device_id=device,
                device_id_type=MESH,
            ),
        )

    def meta_copy(way):
        src, dst, offset, _ = ways[way]
        return pltpu.make_async_remote_copy(
            src_ref=meta.at[src],
            dst_ref=meta.at[dst],
            send_sem=m_send.at[way],
            recv_sem=m_recv.at[dst],
            device_id=(at(offset),),
            device_id_type=MESH,
        )

    def where_sent(way, action):
        if ways[way][3] is None:
            action()
        else:
            pl.when(ways[way][3])(action)

    def send_chunk(way, chunk, with_meta):
        def go():
            if with_meta is True:
                meta_copy(way).start()
            elif with_meta is not False:
                pl.when(with_meta)(lambda: meta_copy(way).start())
            for copy in block_copies(way, chunk):
                copy.start()

        where_sent(way, go)

    first_way = {dst: way for way, (_, dst, _, _) in reversed(list(enumerate(ways)))}

    def got_chunk(slot, chunk):
        for copy in block_copies(first_way[slot], chunk):
            copy.wait_recv()

    def got_meta(slot):
        meta_copy(first_way[slot]).wait_recv()

    def encode(packed):
        most = jnp.maximum(jnp.max(jnp.abs(packed), axis=0, keepdims=True), TINY)
        power = jnp.floor(jnp.log2(SPAN / most))
        times = jnp.exp2(power).astype(jnp.bfloat16).astype(jnp.float32)
        back = jnp.broadcast_to(jnp.exp2(-power), (16, 128))
        return jnp.exp2(packed * times).astype(jnp.bfloat16), back.astype(jnp.bfloat16)

    def decode(ref):
        back = ref[part:, :].astype(jnp.float32)[0:1]
        return jnp.log(ref[:part, :].astype(jnp.float32)) * (back * (1.0 / math.log(2.0)))

    def low_lanes(shape):
        return lax.broadcasted_iota(jnp.int32, shape, 1) < rhs_n

    def vectors(slot, chunk):
        value = decode(dbuf.at[slot, chunk])
        high = value.astype(jnp.bfloat16).astype(jnp.float32)
        low = value - high
        high_r, low_r = pltpu.roll(high, rhs_n, 1), pltpu.roll(low, rhs_n, 1)
        left = low_lanes(value.shape)
        both = jnp.concatenate([jnp.where(left, high, low_r), jnp.where(left, high_r, low)], axis=0)
        top = jnp.concatenate([jnp.where(left, high, 0.0), jnp.where(left, high_r, 0.0)], axis=0)
        return both.astype(jnp.bfloat16), top.astype(jnp.bfloat16)

    def pack_rows(block):
        return jnp.concatenate([block[:, :part], block[:, part:]], axis=0).T

    loads[0].wait()
    scaled = (feat[...].astype(jnp.float32) / lengthscale[...]).astype(jnp.bfloat16)
    xbuf[OWN] = scaled
    exact = scaled.astype(jnp.float32)
    half = 0.5 * jnp.sum(exact * exact, axis=1, keepdims=True)
    half_col[0] = jnp.broadcast_to(half, (pts, 128))
    middle[0] = jnp.mean(half_col[0], axis=0, keepdims=True)
    for r in range(pts // 128):
        meta[OWN, r : r + 1, :] = half_col[0, r * 128 : (r + 1) * 128, :].T[0:1, :]
    loads[1].wait()
    for chunk in range(CHUNKS):
        code, back = encode(pack_rows(dvec[:, chunk * width : (chunk + 1) * width]))
        dbuf[OWN, chunk, :part] = code
        dbuf[OWN, chunk, part:] = back

    pl.semaphore_wait(barrier, len(peers))
    for chunk in range(CHUNKS):
        for way in range(4):
            send_chunk(way, chunk, chunk == 0)

    def gram(left_slot, slot, chunk, par):
        rows = pl.ds(pl.multiple_of(chunk * width, width), width)
        s_buf[par][...] = dot(xbuf[left_slot], xbuf[slot, rows, :], ((1,), (1,)))

    def covariance(u):
        r = u * lax.rsqrt(u)
        return ((r + POLY_P) * r + POLY_Q) * jnp.exp2(r * (-RATE))

    def elem(half_slot, slot, chunk, par):
        for h in range(width // 128):
            row = meta[slot, pl.ds(chunk * (width // 128) + h, 1), :]
            mid = covariance(jnp.maximum(middle[half_slot] + row, TINY))
            centre[par, h : h + 1, :] = mid
            for strip in range(pts // STRIP):
                rows = slice(strip * STRIP, (strip + 1) * STRIP)
                lanes = slice(h * 128, (h + 1) * 128)
                u = (half_col[half_slot, rows, :] + row) - s_buf[par][rows, lanes]
                t_buf[par][rows, lanes] = (covariance(jnp.maximum(u, TINY)) - mid).astype(jnp.bfloat16)

    def forward(total, slot, chunk, par):
        both, top = vectors(slot, chunk)
        mid = jnp.concatenate([centre[par, h : h + 1, :] for h in range(width // 128)], axis=1)
        mid = jnp.broadcast_to(mid, (16, width))
        high = mid.astype(jnp.bfloat16)
        low = (mid - high.astype(jnp.float32)).astype(jnp.bfloat16)
        added = dot(high, both, ((1,), (0,))) + dot(low, top, ((1,), (0,)))
        total[...] += dot(t_buf[par][...], both, ((1,), (0,))) + added[0:1]

    def backward(kind, chunk, par):
        full = dot(dt[...], t_buf[par][...], ((1,), (0,)))
        added = [dsum[...] * centre[par, h : h + 1, :] for h in range(width // 128)]
        code, back = encode(pack_rows(full[:rhs_n] + full[rhs_n:] + jnp.concatenate(added, axis=1)))
        ret_out[kind, chunk, :part] = code
        ret_out[kind, chunk, part:] = back

    def ret_copy(kind, chunk, offset=1):
        return pltpu.make_async_remote_copy(
            src_ref=ret_out.at[kind, chunk],
            dst_ref=ret_in.at[kind, chunk],
            send_sem=r_send.at[kind, chunk],
            recv_sem=r_recv.at[kind, chunk],
            device_id=(at(offset),),
            device_id_type=MESH,
        )

    def transposed(total):
        turned = total[...].T
        return turned[:rhs_n] + turned[rhs_n:]

    def run(left_slot, half_slot, steps, place, total, each_pair=None, kind=None):
        t1[...] = jnp.zeros_like(t1)
        centre[1] = jnp.zeros_like(centre[1])
        gram(left_slot, *place(0), 0)

        @pl.loop(0, steps // 2)
        def _(pair):
            if each_pair is not None:
                each_pair(pair)
            for par in (0, 1):
                step = 2 * pair + par
                gram(left_slot, *place(lax.rem(step + 1, steps)), 1 - par)
                elem(half_slot, *place(step), par)
                before = place(jnp.maximum(step - 1, 0))
                forward(total, *before, 1 - par)
                if kind is not None:
                    backward(kind, before[1], 1 - par)

        final = place(steps - 1)
        forward(total, *final, 1)
        if kind is not None:
            backward(kind, final[1], 1)

    acc[...] = jnp.zeros_like(acc)

    def first_place(step):
        later = (step - CHUNKS) // 2
        if isinstance(step, int):
            return (OWN, step) if step < CHUNKS else (P32 + step % 2, later)
        own = step < CHUNKS
        return jnp.where(own, OWN, P32 + lax.rem(step, 2)), jnp.where(own, step, later)

    def pass_on(slot, chunk, with_meta):
        got_chunk(slot, chunk)
        for way, (src, _, _, _) in enumerate(ways):
            if src == slot:
                send_chunk(way, chunk, with_meta)

    def first_arrivals(pair):
        for slot, lag in ((P32, 1), (M32, 2), (M1, 3)):
            chunk = pair - lag

            @pl.when(jnp.logical_and(chunk >= 0, chunk < CHUNKS))
            def _():
                pl.when(chunk == 0)(lambda: got_meta(slot))
                pass_on(slot, chunk, chunk == 0)

    run(OWN, 0, 3 * CHUNKS, first_place, acc, first_arrivals)
    pass_on(M1, CHUNKS - 1, False)

    for kind, left_slot, slot, back_to, ahead_to in ((0, M32, P33, 33, -32), (2, M2, P1, 1, -2)):
        for late in (P33,) if kind == 0 else (M2, P1):
            got_meta(late)
            for chunk in range(CHUNKS):
                got_chunk(late, chunk)
        for r in range(pts // 128):
            half_col[1, r * 128 : (r + 1) * 128, :] = jnp.broadcast_to(
                meta[left_slot, r : r + 1, :], (128, 128)
            ).T
        for chunk in range(CHUNKS):
            dt[:, chunk * width : (chunk + 1) * width] = vectors(left_slot, chunk)[0].T
        middle[1] = jnp.mean(half_col[1], axis=0, keepdims=True)
        total_d = jnp.sum(dt[...].astype(jnp.float32), axis=1, keepdims=True)
        dsum[...] = jnp.broadcast_to(total_d[:rhs_n] + total_d[rhs_n:], (rhs_n, 128))
        acc2[...] = jnp.zeros_like(acc2)
        run(left_slot, 1, CHUNKS, lambda step, slot=slot: (slot, step), acc2, None, kind)
        for chunk in range(CHUNKS):
            ahead = acc2[chunk * width : (chunk + 1) * width, :]
            ahead = ahead + pltpu.roll(ahead, rhs_n, 1)
            ahead = jnp.where(low_lanes((part, 128)), ahead[:part], ahead[part:])
            code, back = encode(ahead)
            ret_out[kind + 1, chunk, :part] = code
            ret_out[kind + 1, chunk, part:] = back
            ret_copy(kind, chunk, back_to).start()
            ret_copy(kind + 1, chunk, ahead_to).start()

    def last_place(step):
        return step // CHUNKS + P1, step % CHUNKS if isinstance(step, int) else lax.rem(step, CHUNKS)

    run(OWN, 0, 2 * CHUNKS, last_place, acc)

    for kind in range(4):
        for chunk in range(CHUNKS):
            ret_copy(kind, chunk).wait_recv()
    for chunk in range(CHUNKS):
        there = decode(ret_in.at[0, chunk])
        for kind in range(1, 4):
            there = there + decode(ret_in.at[kind, chunk])
        left = low_lanes(there.shape)
        acc[chunk * width : chunk * width + part, :] += jnp.where(left, there, 0.0)
        acc[chunk * width + part : (chunk + 1) * width, :] += jnp.where(left, 0.0, there)
    own_part = transposed(acc)
    loads[2].wait()
    scale = outputscale[0] * (10.0 / 3.0)
    noise = noise_var[0]
    lane_sums = [jnp.zeros((rhs_n, 128), jnp.float32)] * 4
    for chunk in range(CHUNKS):
        lanes = slice(chunk * width, (chunk + 1) * width)
        vec, old = dvec[:, lanes], res[:, lanes]
        applied = noise * vec + scale * own_part[:, lanes]
        applied_ref[:, lanes] = applied
        for at_sum, term in enumerate((old * old, vec * applied, old * applied, applied * applied)):
            for h in range(width // 128):
                lane_sums[at_sum] = lane_sums[at_sum] + term[:, h * 128 : (h + 1) * 128]
    rows = [
        jnp.sum(jnp.concatenate(lane_sums[2 * i : 2 * i + 2], axis=0).T, axis=0, keepdims=True)
        for i in range(2)
    ]
    running = jnp.concatenate(rows + [jnp.zeros((6, 128), jnp.float32)], axis=0)

    base = 0
    for stride, size in stages:
        sums[base] = running
        place = lax.rem(me // stride, size)
        copies = []
        for k in range(1, size):
            copies.append(pltpu.make_async_remote_copy(
                src_ref=sums.at[base],
                dst_ref=sums.at[base + k],
                send_sem=a_send.at[base + k],
                recv_sem=a_recv.at[base + k],
                device_id=(group_peer(stride, size, k),),
                device_id_type=MESH,
            ))
        for copy in copies:
            copy.start()
        for copy in copies:
            copy.wait_recv()
        parts = [sums[base + lax.rem(place - member + size, size)] for member in range(size)]
        running = parts[0]
        for part in parts[1:]:
            running = running + part
        base += size

    mean = running * (1.0 / (n_dev * pts))
    swapped = pltpu.roll(mean, 64, 1)
    old_norm, curvature = mean[0:1], swapped[0:1]
    cross_term, applied_norm = mean[1:2], swapped[1:2]
    step_size = old_norm / jnp.maximum(curvature, 1.0)
    updated = old_norm - 2.0 * step_size * cross_term + step_size * step_size * applied_norm
    ratio = updated / (old_norm + 1e-6)
    coef_ref[...] = jnp.concatenate([step_size, ratio, jnp.zeros((6, 128), jnp.float32)], axis=0)

    for way in range(len(ways)):
        def left(way=way):
            meta_copy(way).wait_send()
            for chunk in range(CHUNKS):
                for copy in block_copies(way, chunk):
                    copy.wait_send()

        where_sent(way, left)
    for kind in range(4):
        for chunk in range(CHUNKS):
            ret_copy(kind, chunk).wait_send()
    base = 0
    for stride, size in stages:
        for k in range(1, size):
            pltpu.make_async_remote_copy(
                src_ref=sums.at[base],
                dst_ref=sums.at[base + k],
                send_sem=a_send.at[base + k],
                recv_sem=a_recv.at[base + k],
                device_id=(me,),
                device_id_type=MESH,
            ).wait_send()
        base += size


def local(n_dev, features, lengthscale, noise_var, outputscale, solution, residual, direction):
    pts, feat_n = features.shape
    rhs_n = direction.shape[1]
    width = pts // CHUNKS
    f32, bf16 = jnp.float32, jnp.bfloat16
    dma = pltpu.SemaphoreType.DMA
    in_place = pl.BlockSpec(memory_space=pltpu.HBM)
    vmem = pl.BlockSpec(memory_space=pltpu.VMEM)
    smem = pl.BlockSpec(memory_space=pltpu.SMEM)
    n_sums = 8 + 4 + n_dev // 32

    def body(*refs):
        kernel(n_dev, width, *refs)

    applied, coef = pl.pallas_call(
        body,
        out_shape=(
            jax.ShapeDtypeStruct((rhs_n, pts), f32),
            jax.ShapeDtypeStruct((8, 128), f32),
        ),
        in_specs=[in_place, vmem, smem, smem, in_place, in_place],
        out_specs=(vmem, vmem),
        scratch_shapes=[
            pltpu.VMEM((pts, feat_n), bf16),
            pltpu.VMEM((rhs_n, pts), f32),
            pltpu.VMEM((rhs_n, pts), f32),
            pltpu.VMEM((7, pts, feat_n), bf16),
            pltpu.VMEM((7, CHUNKS, width // 2 + 16, 128), bf16),
            pltpu.VMEM((7, 8, 128), f32),
            pltpu.VMEM((2, pts, 128), f32),
            pltpu.VMEM((2 * rhs_n, pts), bf16),
            pltpu.VMEM((pts, width), f32),
            pltpu.VMEM((pts, width), f32),
            pltpu.VMEM((pts, width), bf16),
            pltpu.VMEM((pts, width), bf16),
            pltpu.VMEM((2, 1, 128), f32),
            pltpu.VMEM((2, width // 128, 128), f32),
            pltpu.VMEM((rhs_n, 128), f32),
            pltpu.VMEM((pts, 128), f32),
            pltpu.VMEM((pts, 128), f32),
            pltpu.VMEM((4, CHUNKS, width // 2 + 16, 128), bf16),
            pltpu.VMEM((4, CHUNKS, width // 2 + 16, 128), bf16),
            pltpu.VMEM((n_sums, 8, 128), f32),
            dma((3,)),
            dma((9, CHUNKS)),
            dma((7, CHUNKS)),
            dma((9, CHUNKS)),
            dma((7, CHUNKS)),
            dma((9,)),
            dma((7,)),
            dma((4, CHUNKS)),
            dma((4, CHUNKS)),
            dma((n_sums,)),
            dma((n_sums,)),
        ],
        compiler_params=pltpu.CompilerParams(
            collective_id=0, has_side_effects=True, vmem_limit_bytes=60 * 1024 * 1024
        ),
        name="cg_step",
    )(features, lengthscale.reshape(1, feat_n), noise_var, outputscale, direction.T, residual.T)
    applied = applied.T
    step_size, ratio = coef[0, :rhs_n], coef[1, :rhs_n]
    new_solution = solution + step_size[None, :] * direction
    new_residual = residual - step_size[None, :] * applied
    new_direction = new_residual + ratio[None, :] * direction
    return (new_solution, new_residual, new_direction)


def solution(mesh):
    n_dev = mesh.shape[AXIS]
    rows = P(AXIS, None)

    def whole(*arrays):
        return local(n_dev, *arrays)

    return jax.shard_map(
        whole,
        mesh=mesh,
        in_specs=(rows, P(), P(), P(), rows, rows, rows),
        out_specs=(rows, rows, rows),
        check_vma=False,
    )
```
